32 devices in a mesh: replica: 4 (over y, core), fsdp: 8 (over z, x).
Axes of the slice: x: 2, y: 2, z: 4, core: 2. Of those that a mesh axis runs over, the one named last changes fastest.
Arguments:
- layer_input: bfloat16 [2, 4096, 4096], P(None, ('replica', 'fsdp')), may hold values from -6 to 6
- queries: bfloat16 [2, 4096, 4096], P(None, ('replica', 'fsdp')), may hold values from -100 to 100
- keys: bfloat16 [2, 4096, 512], P(None, ('replica', 'fsdp')), may hold values from -8 to 8
- targets: bfloat16 [2, 4096, 4096], P(None, ('replica', 'fsdp')), may hold values from -6 to 6
- value_weight: float32 [4096, 512], P('fsdp'), may hold values from -6 to 6
- outer_momentum: float32 [4096, 512], P('fsdp'), may hold values from -0.6 to 0.6
Outputs:
- new_weight: float32 [4096, 512], P('fsdp')
- new_momentum: float32 [4096, 512], P('fsdp')
The draws below stay inside these ranges and needn't reach their ends.
All inputs are finite; a program needn't handle non-finite values.
Results may differ from the reference program's by a relative error of at most 0.0017.
Values may be sent and summed in bfloat16 or wider, within the bound.
A program may use at most 64 MiB of HBM per device.

```python
import math
import jax
import jax.numpy as jnp
from jax import lax

D = 4096
QH = 32
KVH = 4
HD = 128
STEPS = 2
TOK_DEV = 128
TOKENS = 4096
N_REPLICA = 4
N_FSDP = 8


def attention_pair(seed_key):
    base = jax.random.fold_in(seed_key, 911)
    key_query, key_key = jax.random.split(base, 2)
    sequences = TOKENS // TOK_DEV
    group_size = QH // KVH
    key_rows = jax.random.normal(key_key, (STEPS, sequences, TOK_DEV, KVH, HD), jnp.float32)
    query_rows = jax.random.normal(key_query, (STEPS, sequences, TOK_DEV, KVH, group_size, HD), jnp.float32)
    query_rows = jnp.clip(query_rows, -100.0, 100.0).reshape(STEPS, TOKENS, QH * HD)
    key_rows = jnp.clip(key_rows, -8.0, 8.0).reshape(STEPS, TOKENS, KVH * HD)
    return (query_rows, key_rows)


def draw_queries(key, part):
    return attention_pair(key)[0].astype(jnp.bfloat16)


def draw_keys(key, part):
    return attention_pair(key)[1].astype(jnp.bfloat16)


def shard_levels(key, shape, cuts, least, high):
    loudness, own = 1.0, jax.random.fold_in(key, 6)
    for dim, blocks in cuts:
        heights = jnp.exp(jax.random.uniform(jax.random.fold_in(own, dim), (blocks,), jnp.float32, least / len(cuts), high / len(cuts)))
        loudness = loudness * jnp.repeat(heights, shape[dim] // blocks).reshape([-1 if axis == dim else 1 for axis in range(len(shape))])
    return loudness


def normal_values(stream_key, extent, spread, bound, shards=(), kind=jnp.bfloat16):
    result = spread * jax.random.normal(stream_key, extent, jnp.float32)
    if shards:
        result = result * shard_levels(stream_key, extent, shards, -0.22, 0.18)
    return jnp.clip(result, -bound, bound).astype(kind)


def setup_inputs(seed: int = 0) -> dict:
    arg_keys = jax.random.split(jax.random.key(seed), 7)
    return {
        "layer_input": normal_values(arg_keys[0], (STEPS, TOKENS, D), 1.0, 6.0, ((1, 32),)),
        "queries": draw_queries(jax.random.fold_in(arg_keys[6], 71), 0),
        "keys": draw_keys(jax.random.fold_in(arg_keys[6], 71), 0),
        "targets": normal_values(arg_keys[3], (STEPS, TOKENS, QH * HD), 1.0, 6.0, ((1, 32),)),
        "value_weight": normal_values(arg_keys[4], (D, KVH * HD), 1.0, 6.0, ((0, 8),), jnp.float32),
        "outer_momentum": normal_values(arg_keys[5], (D, KVH * HD), 0.1, 0.6, ((0, 8),), jnp.float32),
    }


beta_one = 0.9
beta_two = 0.95
inner_rate = 0.05
decay_rate = 0.1
outer_rate = 0.7
outer_mu = 0.9

def sequence_grad(query_rows, key_rows, values, target_rows):
    group_size = QH // KVH
    length = query_rows.shape[0]
    query_heads = query_rows.astype(jnp.float32).reshape(length, KVH, group_size, HD)
    key_heads = key_rows.astype(jnp.float32).reshape(length, KVH, HD)
    scores = jnp.einsum('qgjd,kgd->gjqk', query_heads, key_heads) / math.sqrt(HD)
    causal = jnp.arange(length)[:, None] >= jnp.arange(length)[None, :]
    scores = jnp.where(causal, scores, -1e+30)
    highest = lax.optimization_barrier(jnp.max(scores, axis=-1, keepdims=True))
    expd = jnp.exp(scores - highest)
    attention = (expd / lax.optimization_barrier(jnp.sum(expd, axis=-1, keepdims=True))).astype(jnp.bfloat16)
    attn_wide = attention.astype(jnp.float32)
    value_heads = values.astype(jnp.float32).reshape(length, KVH, HD)
    attended = jnp.einsum('gjqk,kgd->qgjd', attn_wide, value_heads).reshape(length, QH * HD)
    out_grad = ((attended - target_rows.astype(jnp.float32)) / (TOK_DEV * N_FSDP)).astype(jnp.bfloat16)
    grad_heads = out_grad.astype(jnp.float32).reshape(length, KVH, group_size, HD)
    value_grad = jnp.einsum('gjqk,qgjd->kgd', attn_wide, grad_heads).reshape(length, KVH * HD)
    return value_grad.astype(jnp.bfloat16)

def replica_round(value_weight, layer_input, queries, keys, targets, replica):
    tok_rep = TOK_DEV * N_FSDP
    adam_floor = math.sqrt(QH // KVH / (tok_rep * D))
    first_row = replica * tok_rep
    weights_now = value_weight
    moment_one = jnp.zeros_like(value_weight)
    moment_two = jnp.zeros_like(value_weight)
    for step_index in range(STEPS):
        inputs = layer_input[step_index, first_row:first_row + tok_rep]
        weights_bf = weights_now.astype(jnp.bfloat16)
        values = (jnp.dot(inputs, weights_bf, preferred_element_type=jnp.float32) / math.sqrt(D)).astype(jnp.bfloat16)
        query_seq = queries[step_index, first_row:first_row + tok_rep].reshape(N_FSDP, TOK_DEV, QH * HD)
        key_seq = keys[step_index, first_row:first_row + tok_rep].reshape(N_FSDP, TOK_DEV, KVH * HD)
        value_seq = values.reshape(N_FSDP, TOK_DEV, KVH * HD)
        target_seq = targets[step_index, first_row:first_row + tok_rep].reshape(N_FSDP, TOK_DEV, QH * HD)
        value_grad = lax.map(lambda group: sequence_grad(group[0], group[1], group[2], group[3]), (query_seq, key_seq, value_seq, target_seq))
        value_grad = value_grad.reshape(tok_rep, KVH * HD)
        gradient = jnp.dot(inputs.T, value_grad, preferred_element_type=jnp.float32) / math.sqrt(D)
        moment_one = beta_one * moment_one + (1.0 - beta_one) * gradient
        moment_two = beta_two * moment_two + (1.0 - beta_two) * gradient * gradient
        corrected_one = moment_one / (1.0 - beta_one ** (step_index + 1))
        corrected_two = moment_two / (1.0 - beta_two ** (step_index + 1))
        weights_now = weights_now - inner_rate * (corrected_one / (jnp.sqrt(corrected_two) + adam_floor) + decay_rate * weights_now)
    return weights_now

def reference(layer_input, queries, keys, targets, value_weight, outer_momentum):
    total_delta = jnp.zeros_like(value_weight)
    for replica in range(N_REPLICA):
        total_delta = total_delta + (value_weight - replica_round(value_weight, layer_input, queries, keys, targets, replica))
    mean_delta = total_delta / N_REPLICA
    new_momentum = outer_mu * outer_momentum + mean_delta
    new_weight = value_weight - outer_rate * (mean_delta + outer_mu * new_momentum)
    return (new_weight, new_momentum)
```

```python
import functools
import math

import jax
import jax.numpy as jnp
from jax import lax
from jax.experimental import pallas as pl
from jax.experimental.pallas import tpu as pltpu
from jax.sharding import PartitionSpec as P

D = 4096
QH = 32
KVH = 4
HD = 128


beta_one = 0.9
beta_two = 0.95
inner_rate = 0.05
decay_rate = 0.1
outer_rate = 0.7
outer_mu = 0.9


def plain_shards(layer_input, queries, keys, targets, value_weight, outer_momentum):
    inner_steps = layer_input.shape[0]
    length = layer_input.shape[1]
    columns = value_weight.shape[1]
    fsdp_count = lax.axis_size("fsdp")
    replicas = lax.axis_size("replica")
    tok_rep = length * fsdp_count
    group_size = QH // KVH
    adam_floor = math.sqrt(group_size / (tok_rep * D))
    by_features = lax.all_to_all(layer_input, "fsdp", split_axis=2, concat_axis=1, tiled=True)
    causal = jnp.arange(length)[:, None] >= jnp.arange(length)[None, :]
    weights_now = value_weight
    moment_one = jnp.zeros_like(value_weight)
    moment_two = jnp.zeros_like(value_weight)
    for step_index in range(inner_steps):
        inputs = layer_input[step_index]
        shard_bf = weights_now.astype(jnp.bfloat16)
        product = jnp.dot(
            inputs,
            lax.all_gather(shard_bf, "fsdp", axis=0, tiled=True),
            preferred_element_type=jnp.float32,
        )
        values = (product / math.sqrt(D)).astype(jnp.bfloat16)
        query_heads = queries[step_index].reshape(length, KVH, group_size, HD)
        key_heads = keys[step_index].reshape(length, KVH, HD)
        scores = jnp.einsum(
            "qgjd,kgd->gjqk", query_heads, key_heads, preferred_element_type=jnp.float32
        ) / math.sqrt(HD)
        scores = jnp.where(causal, scores, -1e30)
        highest = jnp.max(scores, axis=-1, keepdims=True)
        expd = jnp.exp(scores - highest)
        attention = (expd / jnp.sum(expd, axis=-1, keepdims=True)).astype(jnp.bfloat16)
        attended = jnp.einsum(
            "gjqk,kgd->qgjd",
            attention,
            values.reshape(length, KVH, HD),
            preferred_element_type=jnp.float32,
        ).reshape(length, QH * HD)
        out_grad = ((attended - targets[step_index].astype(jnp.float32)) / tok_rep).astype(
            jnp.bfloat16
        )
        value_grad = (
            jnp.einsum(
                "gjqk,qgjd->kgd",
                attention,
                out_grad.reshape(length, KVH, group_size, HD),
                preferred_element_type=jnp.float32,
            )
            .reshape(length, columns)
            .astype(jnp.bfloat16)
        )
        step_features = by_features[step_index]
        gradient = lax.dot_general(
            step_features,
            lax.all_gather(value_grad, "fsdp", axis=0, tiled=True),
            (((0,), (0,)), ((), ())),
            preferred_element_type=jnp.float32,
        ) / math.sqrt(D)
        moment_one = beta_one * moment_one + (1.0 - beta_one) * gradient
        moment_two = beta_two * moment_two + (1.0 - beta_two) * gradient * gradient
        corrected_one = moment_one / (1.0 - beta_one ** (step_index + 1))
        corrected_two = moment_two / (1.0 - beta_two ** (step_index + 1))
        weights_now = weights_now - inner_rate * (
            corrected_one / (jnp.sqrt(corrected_two) + adam_floor) + decay_rate * weights_now
        )
    total_delta = lax.psum(value_weight - weights_now, "replica")
    mean_delta = total_delta / replicas
    new_momentum = outer_mu * outer_momentum + mean_delta
    new_weight = value_weight - outer_rate * (mean_delta + outer_mu * new_momentum)
    return (new_weight, new_momentum)


MESH = pl.DeviceIdType.MESH


def round_kernel(
    n,
    x_ref,
    q_ref,
    k_ref,
    t_ref,
    w_ref,
    om_ref,
    nw_ref,
    nm_ref,
    feat,
    mat_hi,
    mat_lo,
    base,
    side_out,
    side_in,
    col_out,
    col_in,
    vgrad,
    grad,
    theta,
    mom_one,
    mom_two,
    wbf,
    acc,
    delta,
    core_in,
    pair_out,
    pair_in,
    total,
    in_s,
    in_r,
    side_s,
    side_r,
    col_s,
    col_r,
    agz_s,
    agz_r,
    agx_s,
    agx_r,
    rep_s,
    rep_r,
):
    steps, length, _ = x_ref.shape
    rows, columns = w_ref.shape
    heads = columns // HD
    group = QH // KVH
    tok_rep = length * n
    adam_floor = math.sqrt(group / (tok_rep * D))
    nz = n // 2
    me = lax.axis_index("fsdp")
    rep = lax.axis_index("replica")
    z, px = me // 2, me % 2
    core = rep % 2
    core_peer = rep + 1 - 2 * core
    pair_peer = (rep + 2) % 4
    side = z * 2 + (1 - px)

    def at(dz, dx):
        return ((z + dz + nz) % nz) * 2 + (px + dx) % 2

    hops = [(dz, 1) for dz in range(nz)] + [(dz, 0) for dz in range(1, nz)]

    barrier = pltpu.get_barrier_semaphore()
    for dz, dx in hops:
        pl.semaphore_signal(barrier, inc=1, device_id={"fsdp": at(dz, dx)}, device_id_type=MESH)
    for peer in (core_peer, pair_peer):
        pl.semaphore_signal(barrier, inc=1, device_id={"replica": peer}, device_id_type=MESH)
    pl.semaphore_wait(barrier, n + 1)

    def send(src, dst, ssem, rsem, axis, peer):
        copy = pltpu.make_async_remote_copy(
            src_ref=src,
            dst_ref=dst,
            send_sem=ssem,
            recv_sem=rsem,
            device_id={axis: peer},
            device_id_type=MESH,
        )
        copy.start()
        return copy

    def send_inputs(s):
        copies = {}
        for dz, dx in hops:
            peer = at(dz, dx)
            i = dz * 2 + dx
            copies[dz, dx] = send(
                x_ref.at[s, :, pl.ds(pl.multiple_of(peer * rows, 128), rows)],
                feat.at[s, me],
                in_s.at[s, i],
                in_r.at[s, i],
                "fsdp",
                peer,
            )
        return copies

    causal = lax.broadcasted_iota(jnp.int32, (length, length), 0) >= lax.broadcasted_iota(
        jnp.int32, (length, length), 1
    )

    def attention_of(s):
        def one(g, carry):
            keys = k_ref[s, :, pl.ds(pl.multiple_of(g * HD, HD), HD)]
            both = jnp.zeros((length, length + HD), jnp.float32)
            for j in range(group):
                cols = pl.ds(pl.multiple_of((g * group + j) * HD, HD), HD)
                scores = lax.dot_general(
                    q_ref[s, :, cols],
                    keys,
                    (((1,), (1,)), ((), ())),
                    preferred_element_type=jnp.float32,
                ) / math.sqrt(HD)
                scores = jnp.where(causal, scores, -1e30)
                highest = jnp.max(scores, axis=-1, keepdims=True)
                expd = jnp.exp(scores - highest)
                att = (expd / jnp.sum(expd, axis=-1, keepdims=True)).astype(jnp.bfloat16)
                both += lax.dot_general(
                    att,
                    jnp.concatenate([att, t_ref[s, :, cols]], axis=1),
                    (((0,), (0,)), ((), ())),
                    preferred_element_type=jnp.float32,
                )
            gram = both[:, :length]
            high = gram.astype(jnp.bfloat16)
            mat_hi[s, g] = high
            mat_lo[s, g] = (gram - high.astype(jnp.float32)).astype(jnp.bfloat16)
            base[s, g] = both[:, length:]
            return carry

        lax.fori_loop(0, heads, one, 0)

    chunk = 32

    def chunks(body):
        def step(i, carry):
            body(pl.ds(pl.multiple_of(i * chunk, chunk), chunk))
            return carry

        lax.fori_loop(0, rows // chunk, step, 0)

    pending = []
    inputs = {0: send_inputs(0)}
    for s in range(steps):
        feat[s, me] = x_ref[s, :, pl.ds(pl.multiple_of(me * rows, 128), rows)]

    def cast_weights(c):
        wbf[c, :] = w_ref[c, :].astype(jnp.bfloat16)

    chunks(cast_weights)
    for s in range(steps):
        attention_of(s)

    for s in range(steps):
        def partial(j):
            return jnp.dot(feat[s, j], wbf[...], preferred_element_type=jnp.float32)

        def wait_input(dz, dx):
            inputs[s][(nz - dz) % nz, dx].wait_recv()

        sides = []
        for dz in range(nz):
            wait_input(dz, 1)
            side_out[s, dz] = partial(at(dz, 1)).astype(jnp.bfloat16)
            sides.append(
                send(
                    side_out.at[s, dz],
                    side_in.at[s, dz],
                    side_s.at[s, dz],
                    side_r.at[s, dz],
                    "fsdp",
                    side,
                )
            )
        cols = []
        for dz in list(range(1, nz)) + [0]:
            if dz:
                wait_input(dz, 0)
            own = partial(at(dz, 0))
            sides[dz].wait_recv()
            own = own + side_in[s, dz].astype(jnp.float32)
            if dz:
                col_out[s, dz] = own.astype(jnp.bfloat16)
                cols.append(
                    send(
                        col_out.at[s, dz],
                        col_in.at[s, dz],
                        col_s.at[s, dz],
                        col_r.at[s, dz],
                        "fsdp",
                        at(dz, 0),
                    )
                )
            else:
                acc[...] = own
        if s + 1 < steps:
            inputs[s + 1] = send_inputs(s + 1)
        for dz in range(1, nz):
            cols[dz - 1].wait_recv()
        pending += sides + cols + list(inputs[s].values())

        summed = acc[...]
        for dz in range(1, nz):
            summed = summed + col_in[s, dz].astype(jnp.float32)
        values = (summed / math.sqrt(D)).astype(jnp.bfloat16)
        for g in range(heads):
            part = values[:, g * HD : (g + 1) * HD]
            vg = jnp.dot(mat_hi[s, g], part, preferred_element_type=jnp.float32)
            vg += jnp.dot(mat_lo[s, g], part, preferred_element_type=jnp.float32)
            vg = (vg - base[s, g]) / tok_rep
            vgrad[s, me, :, g * HD : (g + 1) * HD] = vg.astype(jnp.bfloat16)

        def add_block(j, first=False):
            term = lax.dot_general(
                feat[s, j],
                vgrad[s, j],
                (((0,), (0,)), ((), ())),
                preferred_element_type=jnp.float32,
            )
            if first:
                grad[...] = term
            else:
                grad[...] += term

        zs = []
        for dz in range(1, nz):
            zs.append(
                send(
                    vgrad.at[s, me],
                    vgrad.at[s, me],
                    agz_s.at[s, dz],
                    agz_r.at[s, dz],
                    "fsdp",
                    at(dz, 0),
                )
            )
        xs = [
            send(
                vgrad.at[s, me], vgrad.at[s, me], agx_s.at[s, 0], agx_r.at[s, 0], "fsdp", side
            )
        ]
        add_block(me, True)
        for dz in (1, *range(nz - 1, 1, -1)):
            j = at(-dz, 0)
            zs[dz - 1].wait_recv()
            xs.append(
                send(
                    vgrad.at[s, j],
                    vgrad.at[s, j],
                    agx_s.at[s, dz],
                    agx_r.at[s, dz],
                    "fsdp",
                    side,
                )
            )
            add_block(j)
        for i, dz in enumerate((0, 1, *range(nz - 1, 1, -1))):
            xs[i].wait_recv()
            add_block(at(-dz, 1))
        pending += zs + xs

        def adam(c):
            gradient = grad[c, :] / math.sqrt(D)
            one = (1.0 - beta_one) * gradient
            two = (1.0 - beta_two) * gradient * gradient
            if s:
                one = beta_one * mom_one[c, :] + one
                two = beta_two * mom_two[c, :] + two
            now = theta[c, :] if s else w_ref[c, :]
            fixed_one = one / (1.0 - beta_one ** (s + 1))
            fixed_two = two / (1.0 - beta_two ** (s + 1))
            now = now - inner_rate * (
                fixed_one / (jnp.sqrt(fixed_two) + adam_floor) + decay_rate * now
            )
            if s + 1 < steps:
                mom_one[c, :] = one
                mom_two[c, :] = two
                theta[c, :] = now
                wbf[c, :] = now.astype(jnp.bfloat16)
            else:
                delta[c, :] = w_ref[c, :] - now

        chunks(adam)

    half = rows // 2
    mine = pl.ds(pl.multiple_of(core * half, 128), half)
    other = pl.ds(pl.multiple_of((1 - core) * half, 128), half)
    first = send(delta.at[other], core_in, rep_s.at[0], rep_r.at[0], "replica", core_peer)
    first.wait_recv()
    pair_out[...] = (delta[mine, :] + core_in[...]).astype(jnp.bfloat16)
    second = send(pair_out, pair_in, rep_s.at[1], rep_r.at[1], "replica", pair_peer)
    second.wait_recv()
    total[mine, :] = pair_out[...].astype(jnp.float32) + pair_in[...].astype(jnp.float32)
    third = send(
        total.at[mine], total.at[mine], rep_s.at[2], rep_r.at[2], "replica", core_peer
    )

    def finish(start):
        def step(i, carry):
            c = pl.ds(pl.multiple_of(start + i * chunk, chunk), chunk)
            mean = total[c, :] / 4
            momentum = outer_mu * om_ref[c, :] + mean
            nm_ref[c, :] = momentum
            nw_ref[c, :] = w_ref[c, :] - outer_rate * (mean + outer_mu * momentum)
            return carry

        lax.fori_loop(0, half // chunk, step, 0)

    finish(core * half)
    third.wait_recv()
    finish((1 - core) * half)
    for copy in pending + [first, second, third]:
        copy.wait_send()


def shards(layer_input, queries, keys, targets, value_weight, outer_momentum):
    n = lax.axis_size("fsdp")
    replicas = lax.axis_size("replica")
    rows, columns = value_weight.shape
    steps, length, _ = layer_input.shape
    if rows % 256 or n % 2 or replicas != 4 or length % 128:
        return plain_shards(layer_input, queries, keys, targets, value_weight, outer_momentum)
    nz = n // 2
    heads = columns // HD
    bf, f32 = jnp.bfloat16, jnp.float32
    dma = pltpu.SemaphoreType.DMA
    out = jax.ShapeDtypeStruct((rows, columns), f32)
    return pl.pallas_call(
        functools.partial(round_kernel, n),
        out_shape=(out, out),
        in_specs=[pl.BlockSpec(memory_space=pltpu.VMEM)] * 6,
        out_specs=(pl.BlockSpec(memory_space=pltpu.VMEM),) * 2,
        scratch_shapes=[
            pltpu.VMEM((steps, n, length, rows), bf),
            pltpu.VMEM((steps, heads, length, length), bf),
            pltpu.VMEM((steps, heads, length, length), bf),
            pltpu.VMEM((steps, heads, length, HD), f32),
            pltpu.VMEM((steps, nz, length, columns), bf),
            pltpu.VMEM((steps, nz, length, columns), bf),
            pltpu.VMEM((steps, nz, length, columns), bf),
            pltpu.VMEM((steps, nz, length, columns), bf),
            pltpu.VMEM((steps, n, length, columns), bf),
            pltpu.VMEM((rows, columns), f32),
            pltpu.VMEM((rows, columns), f32),
            pltpu.VMEM((rows, columns), f32),
            pltpu.VMEM((rows, columns), f32),
            pltpu.VMEM((rows, columns), bf),
            pltpu.VMEM((length, columns), f32),
            pltpu.VMEM((rows, columns), f32),
            pltpu.VMEM((rows // 2, columns), f32),
            pltpu.VMEM((rows // 2, columns), bf),
            pltpu.VMEM((rows // 2, columns), bf),
            pltpu.VMEM((rows, columns), f32),
            dma((steps, n)),
            dma((steps, n)),
            dma((steps, nz)),
            dma((steps, nz)),
            dma((steps, nz)),
            dma((steps, nz)),
            dma((steps, nz)),
            dma((steps, nz)),
            dma((steps, nz)),
            dma((steps, nz)),
            dma((3,)),
            dma((3,)),
        ],
        compiler_params=pltpu.CompilerParams(collective_id=0, has_side_effects=True),
    )(layer_input, queries, keys, targets, value_weight, outer_momentum)


def solution(mesh):
    in_specs = (
        P(None, ("replica", "fsdp"), None),
        P(None, ("replica", "fsdp"), None),
        P(None, ("replica", "fsdp"), None),
        P(None, ("replica", "fsdp"), None),
        P("fsdp", None),
        P("fsdp", None),
    )
    out_specs = (P("fsdp", None), P("fsdp", None))
    return jax.shard_map(shards, mesh=mesh, in_specs=in_specs, out_specs=out_specs, check_vma=False)
```

```python
import functools
import math

import jax
import jax.numpy as jnp
from jax import lax
from jax.experimental import pallas as pl
from jax.experimental.pallas import tpu as pltpu
from jax.sharding import PartitionSpec as P

D = 4096
QH = 32
KVH = 4
HD = 128


beta_one = 0.9
beta_two = 0.95
inner_rate = 0.05
decay_rate = 0.1
outer_rate = 0.7
outer_mu = 0.9


def plain_shards(layer_input, queries, keys, targets, value_weight, outer_momentum):
    inner_steps = layer_input.shape[0]
    length = layer_input.shape[1]
    columns = value_weight.shape[1]
    fsdp_count = lax.axis_size("fsdp")
    replicas = lax.axis_size("replica")
    tok_rep = length * fsdp_count
    group_size = QH // KVH
    adam_floor = math.sqrt(group_size / (tok_rep * D))
    by_features = lax.all_to_all(layer_input, "fsdp", split_axis=2, concat_axis=1, tiled=True)
    causal = jnp.arange(length)[:, None] >= jnp.arange(length)[None, :]
    weights_now = value_weight
    moment_one = jnp.zeros_like(value_weight)
    moment_two = jnp.zeros_like(value_weight)
    for step_index in range(inner_steps):
        inputs = layer_input[step_index]
        shard_bf = weights_now.astype(jnp.bfloat16)
        product = jnp.dot(
            inputs,
            lax.all_gather(shard_bf, "fsdp", axis=0, tiled=True),
            preferred_element_type=jnp.float32,
        )
        values = (product / math.sqrt(D)).astype(jnp.bfloat16)
        query_heads = queries[step_index].reshape(length, KVH, group_size, HD)
        key_heads = keys[step_index].reshape(length, KVH, HD)
        scores = jnp.einsum(
            "qgjd,kgd->gjqk", query_heads, key_heads, preferred_element_type=jnp.float32
        ) / math.sqrt(HD)
        scores = jnp.where(causal, scores, -1e30)
        highest = jnp.max(scores, axis=-1, keepdims=True)
        expd = jnp.exp(scores - highest)
        attention = (expd / jnp.sum(expd, axis=-1, keepdims=True)).astype(jnp.bfloat16)
        attended = jnp.einsum(
            "gjqk,kgd->qgjd",
            attention,
            values.reshape(length, KVH, HD),
            preferred_element_type=jnp.float32,
        ).reshape(length, QH * HD)
        out_grad = ((attended - targets[step_index].astype(jnp.float32)) / tok_rep).astype(
            jnp.bfloat16
        )
        value_grad = (
            jnp.einsum(
                "gjqk,qgjd->kgd",
                attention,
                out_grad.reshape(length, KVH, group_size, HD),
                preferred_element_type=jnp.float32,
            )
            .reshape(length, columns)
            .astype(jnp.bfloat16)
        )
        step_features = by_features[step_index]
        gradient = lax.dot_general(
            step_features,
            lax.all_gather(value_grad, "fsdp", axis=0, tiled=True),
            (((0,), (0,)), ((), ())),
            preferred_element_type=jnp.float32,
        ) / math.sqrt(D)
        moment_one = beta_one * moment_one + (1.0 - beta_one) * gradient
        moment_two = beta_two * moment_two + (1.0 - beta_two) * gradient * gradient
        corrected_one = moment_one / (1.0 - beta_one ** (step_index + 1))
        corrected_two = moment_two / (1.0 - beta_two ** (step_index + 1))
        weights_now = weights_now - inner_rate * (
            corrected_one / (jnp.sqrt(corrected_two) + adam_floor) + decay_rate * weights_now
        )
    total_delta = lax.psum(value_weight - weights_now, "replica")
    mean_delta = total_delta / replicas
    new_momentum = outer_mu * outer_momentum + mean_delta
    new_weight = value_weight - outer_rate * (mean_delta + outer_mu * new_momentum)
    return (new_weight, new_momentum)


MESH = pl.DeviceIdType.MESH


def round_kernel(
    n,
    x_ref,
    q_ref,
    k_ref,
    t_ref,
    w_ref,
    mean_ref,
    feat,
    q_buf,
    k_buf,
    t_buf,
    w_buf,
    mat_hi,
    mat_lo,
    base,
    side_out,
    side_in,
    col_out,
    col_in,
    vgrad,
    grad,
    theta,
    mom_one,
    mom_two,
    wbf,
    acc,
    delta,
    core_in,
    pair_out,
    pair_in,
    total,
    in_s,
    in_r,
    side_s,
    side_r,
    col_s,
    col_r,
    agz_s,
    agz_r,
    agx_s,
    agx_r,
    rep_s,
    rep_r,
    load_s,
):
    steps, length, _ = x_ref.shape
    rows, columns = w_ref.shape
    parts = 2
    width = columns // parts
    wide = [slice(p * width, (p + 1) * width) for p in range(parts)]
    heads = columns // HD
    group = QH // KVH
    tok_rep = length * n
    adam_floor = math.sqrt(group / (tok_rep * D))
    nz = n // 2
    me = lax.axis_index("fsdp")
    rep = lax.axis_index("replica")
    z, px = me // 2, me % 2
    core = rep % 2
    core_peer = rep + 1 - 2 * core
    pair_peer = (rep + 2) % 4
    side = z * 2 + (1 - px)

    def at(dz, dx):
        return ((z + dz + nz) % nz) * 2 + (px + dx) % 2

    def turn(i):
        return (1 - core) * i + core * (nz - i) if i else 0

    order = [*range(1, nz), 0]
    hops = [(i, 1) for i in order] + [(i, 0) for i in range(1, nz)]

    loads = {}

    def load(i, src, dst):
        loads[i] = pltpu.make_async_copy(src, dst, load_s.at[i])
        loads[i].start()

    barrier = pltpu.get_barrier_semaphore()
    for dz, dx in hops:
        pl.semaphore_signal(barrier, inc=1, device_id={"fsdp": at(dz, dx)}, device_id_type=MESH)
    for peer in (core_peer, pair_peer):
        pl.semaphore_signal(barrier, inc=1, device_id={"replica": peer}, device_id_type=MESH)
    load(steps, q_ref, q_buf)
    load(steps + 1, k_ref, k_buf)
    load(steps + 2, t_ref, t_buf)
    load(steps + 3, w_ref, w_buf)
    pl.semaphore_wait(barrier, n + 1)

    def send(src, dst, ssem, rsem, axis, peer):
        copy = pltpu.make_async_remote_copy(
            src_ref=src,
            dst_ref=dst,
            send_sem=ssem,
            recv_sem=rsem,
            device_id={axis: peer},
            device_id_type=MESH,
        )
        copy.start()
        return copy

    def send_inputs(s, only=None):
        copies = {}
        for k, dx in only or hops:
            dz = turn(k)
            peer = at(dz, dx)
            i = dz * 2 + dx
            copies[k, dx] = send(
                x_ref.at[s, :, pl.ds(pl.multiple_of(peer * rows, 128), rows)],
                feat.at[s, me],
                in_s.at[s, i],
                in_r.at[s, i],
                "fsdp",
                peer,
            )
        return copies

    causal = lax.broadcasted_iota(jnp.int32, (length, length), 0) >= lax.broadcasted_iota(
        jnp.int32, (length, length), 1
    )

    def attention_of(s):
        def one(g, carry):
            keys = k_buf[s, :, pl.ds(pl.multiple_of(g * HD, HD), HD)]
            both = jnp.zeros((length, length + HD), jnp.float32)
            for j in range(group):
                cols = pl.ds(pl.multiple_of((g * group + j) * HD, HD), HD)
                scores = lax.dot_general(
                    q_buf[s, :, cols],
                    keys,
                    (((1,), (1,)), ((), ())),
                    preferred_element_type=jnp.float32,
                ) / math.sqrt(HD)
                scores = jnp.where(causal, scores, -1e30)
                highest = jnp.max(scores, axis=-1, keepdims=True)
                expd = jnp.exp(scores - highest)
                att = (expd / jnp.sum(expd, axis=-1, keepdims=True)).astype(jnp.bfloat16)
                both += lax.dot_general(
                    att,
                    jnp.concatenate([att, t_buf[s, :, cols]], axis=1),
                    (((0,), (0,)), ((), ())),
                    preferred_element_type=jnp.float32,
                )
            gram = both[:, :length]
            high = gram.astype(jnp.bfloat16)
            mat_hi[s, g] = high
            mat_lo[s, g] = (gram - high.astype(jnp.float32)).astype(jnp.bfloat16)
            base[s, g] = both[:, length:]
            return carry

        lax.fori_loop(0, heads, one, 0)

    chunk = 32

    def chunks(body):
        def step(i, carry):
            body(pl.ds(pl.multiple_of(i * chunk, chunk), chunk))
            return carry

        lax.fori_loop(0, rows // chunk, step, 0)

    pending = []
    inputs = {0: send_inputs(0)}
    for s in range(steps):
        load(
            s,
            x_ref.at[s, :, pl.ds(pl.multiple_of(me * rows, 128), rows)],
            feat.at[s, me],
        )

    def cast_weights(c):
        wbf[c, :] = w_buf[c, :].astype(jnp.bfloat16)

    loads[steps + 3].wait()
    chunks(cast_weights)
    for i in (*range(steps), steps, steps + 1, steps + 2):
        loads[i].wait()
    for s in range(steps):
        attention_of(s)

    for s in range(steps):
        def partial(j, p):
            return jnp.dot(feat[s, j], wbf[:, wide[p]], preferred_element_type=jnp.float32)

        if s + 1 < steps:
            inputs[s + 1] = send_inputs(s + 1, hops[:2])
        sides = {}
        for k in order:
            inputs[s][k, 1].wait_recv()
            dz = (nz - turn(k)) % nz if k else 0
            for p in range(parts):
                side_out[s, dz, :, wide[p]] = partial(at(dz, 1), p).astype(jnp.bfloat16)
                sides[k, p] = send(
                    side_out.at[s, dz, :, wide[p]],
                    side_in.at[s, dz, :, wide[p]],
                    side_s.at[s, dz, p],
                    side_r.at[s, dz, p],
                    "fsdp",
                    side,
                )
        cols = {}
        for k in order:
            dz = (nz - turn(k)) % nz if k else 0
            if k:
                inputs[s][k, 0].wait_recv()
            for p in range(parts):
                own = partial(at(dz, 0), p)
                sides[k, p].wait_recv()
                own = own + side_in[s, dz, :, wide[p]].astype(jnp.float32)
                if k:
                    col_out[s, dz, :, wide[p]] = own.astype(jnp.bfloat16)
                    cols[k, p] = send(
                        col_out.at[s, dz, :, wide[p]],
                        col_in.at[s, dz, :, wide[p]],
                        col_s.at[s, dz, p],
                        col_r.at[s, dz, p],
                        "fsdp",
                        at(dz, 0),
                    )
                else:
                    acc[:, wide[p]] = own
        pending += [*sides.values(), *cols.values(), *inputs[s].values()]

        def add_block(j, p, first=False):
            term = lax.dot_general(
                feat[s, j],
                vgrad[s, j, :, wide[p]],
                (((0,), (0,)), ((), ())),
                preferred_element_type=jnp.float32,
            )
            if first:
                grad[:, wide[p]] = term
            else:
                grad[:, wide[p]] += term

        def forward(j, i, p):
            block = vgrad.at[s, j, :, wide[p]]
            return send(block, block, agx_s.at[s, i, p], agx_r.at[s, i, p], "fsdp", side)

        zs = {}
        xs = {}
        for p in range(parts):
            summed = acc[:, wide[p]]
            for k in range(1, nz):
                cols[k, p].wait_recv()
            for dz in range(1, nz):
                summed = summed + col_in[s, dz, :, wide[p]].astype(jnp.float32)
            values = (summed / math.sqrt(D)).astype(jnp.bfloat16)
            for i in range(width // HD):
                g = p * (width // HD) + i
                part = values[:, i * HD : (i + 1) * HD]
                vg = jnp.dot(mat_hi[s, g], part, preferred_element_type=jnp.float32)
                vg += jnp.dot(mat_lo[s, g], part, preferred_element_type=jnp.float32)
                vg = (vg - base[s, g]) / tok_rep
                vgrad[s, me, :, g * HD : (g + 1) * HD] = vg.astype(jnp.bfloat16)
            block = vgrad.at[s, me, :, wide[p]]
            for k in range(1, nz):
                dz = turn(k)
                zs[k, p] = send(
                    block, block, agz_s.at[s, dz, p], agz_r.at[s, dz, p], "fsdp", at(dz, 0)
                )
            xs[0, p] = forward(me, 0, p)
        for p in range(parts):
            add_block(me, p, True)
        for p in range(parts):
            for k in range(1, nz):
                zs[k, p].wait_recv()
                xs[k, p] = forward(at(-turn(k), 0), turn(k), p)
                add_block(at(-turn(k), 0), p)
        if s + 1 < steps:
            inputs[s + 1].update(send_inputs(s + 1, hops[2:]))
        for p in range(parts):
            for k in range(nz):
                xs[k, p].wait_recv()
                add_block(at(-turn(k), 1), p)
        pending += [*zs.values(), *xs.values()]

        def adam(c):
            gradient = grad[c, :] / math.sqrt(D)
            one = (1.0 - beta_one) * gradient
            two = (1.0 - beta_two) * gradient * gradient
            if s:
                one = beta_one * mom_one[c, :] + one
                two = beta_two * mom_two[c, :] + two
            now = theta[c, :] if s else w_buf[c, :]
            fixed_one = one / (1.0 - beta_one ** (s + 1))
            fixed_two = two / (1.0 - beta_two ** (s + 1))
            now = now - inner_rate * (
                fixed_one / (jnp.sqrt(fixed_two) + adam_floor) + decay_rate * now
            )
            if s + 1 < steps:
                mom_one[c, :] = one
                mom_two[c, :] = two
                theta[c, :] = now
                wbf[c, :] = now.astype(jnp.bfloat16)
            else:
                delta[c, :] = w_buf[c, :] - now

        if s + 1 < steps:
            chunks(adam)

    half = rows // 2
    piece = half // parts

    def span(which, p):
        return pl.multiple_of(which * half + p * piece, 128)

    def over(start, body):
        def step(i, carry):
            body(pl.ds(pl.multiple_of(start + i * chunk, chunk), chunk))
            return carry

        lax.fori_loop(0, piece // chunk, step, 0)

    first, second, third = [], [], []
    for p in range(parts):
        over(span(1 - core, p), adam)
        first.append(
            send(
                delta.at[pl.ds(span(1 - core, p), piece)],
                core_in.at[pl.ds(p * piece, piece)],
                rep_s.at[0, p],
                rep_r.at[0, p],
                "replica",
                core_peer,
            )
        )
    for p in range(parts):
        over(span(core, p), adam)
        first[p].wait_recv()
        rows_p = pl.ds(p * piece, piece)
        pair_out[rows_p, :] = (
            delta[pl.ds(span(core, p), piece), :] + core_in[rows_p, :]
        ).astype(jnp.bfloat16)
        second.append(
            send(
                pair_out.at[rows_p],
                pair_in.at[rows_p],
                rep_s.at[1, p],
                rep_r.at[1, p],
                "replica",
                pair_peer,
            )
        )

    def finish(c):
        mean_ref[c, :] = total[c, :] / 4

    for p in range(parts):
        second[p].wait_recv()
        rows_p = pl.ds(p * piece, piece)
        mine = pl.ds(span(core, p), piece)
        total[mine, :] = pair_out[rows_p, :].astype(jnp.float32) + pair_in[
            rows_p, :
        ].astype(jnp.float32)
        third.append(
            send(
                total.at[mine],
                total.at[mine],
                rep_s.at[2, p],
                rep_r.at[2, p],
                "replica",
                core_peer,
            )
        )
        over(span(core, p), finish)
    for p in range(parts):
        third[p].wait_recv()
        over(span(1 - core, p), finish)
    for copy in pending + first + second + third:
        copy.wait_send()


def shards(layer_input, queries, keys, targets, value_weight, outer_momentum):
    n = lax.axis_size("fsdp")
    replicas = lax.axis_size("replica")
    rows, columns = value_weight.shape
    steps, length, _ = layer_input.shape
    if rows % 512 or columns % (2 * HD) or n % 2 or replicas != 4 or length % 128:
        return plain_shards(layer_input, queries, keys, targets, value_weight, outer_momentum)
    nz = n // 2
    heads = columns // HD
    bf, f32 = jnp.bfloat16, jnp.float32
    dma = pltpu.SemaphoreType.DMA
    out = jax.ShapeDtypeStruct((rows, columns), f32)
    mean_delta = pl.pallas_call(
        functools.partial(round_kernel, n),
        out_shape=out,
        in_specs=[pl.BlockSpec(memory_space=pl.ANY)] * 5,
        out_specs=pl.BlockSpec(memory_space=pltpu.VMEM),
        scratch_shapes=[
            pltpu.VMEM((steps, n, length, rows), bf),
            pltpu.VMEM(queries.shape, bf),
            pltpu.VMEM(keys.shape, bf),
            pltpu.VMEM(targets.shape, bf),
            pltpu.VMEM((rows, columns), f32),
            pltpu.VMEM((steps, heads, length, length), bf),
            pltpu.VMEM((steps, heads, length, length), bf),
            pltpu.VMEM((steps, heads, length, HD), f32),
            pltpu.VMEM((steps, nz, length, columns), bf),
            pltpu.VMEM((steps, nz, length, columns), bf),
            pltpu.VMEM((steps, nz, length, columns), bf),
            pltpu.VMEM((steps, nz, length, columns), bf),
            pltpu.VMEM((steps, n, length, columns), bf),
            pltpu.VMEM((rows, columns), f32),
            pltpu.VMEM((rows, columns), f32),
            pltpu.VMEM((rows, columns), f32),
            pltpu.VMEM((rows, columns), f32),
            pltpu.VMEM((rows, columns), bf),
            pltpu.VMEM((length, columns), f32),
            pltpu.VMEM((rows, columns), f32),
            pltpu.VMEM((rows // 2, columns), f32),
            pltpu.VMEM((rows // 2, columns), bf),
            pltpu.VMEM((rows // 2, columns), bf),
            pltpu.VMEM((rows, columns), f32),
            dma((steps, n)),
            dma((steps, n)),
            dma((steps, nz, 2)),
            dma((steps, nz, 2)),
            dma((steps, nz, 2)),
            dma((steps, nz, 2)),
            dma((steps, nz, 2)),
            dma((steps, nz, 2)),
            dma((steps, nz, 2)),
            dma((steps, nz, 2)),
            dma((3, 2)),
            dma((3, 2)),
            dma((steps + 4,)),
        ],
        compiler_params=pltpu.CompilerParams(collective_id=0, has_side_effects=True),
    )(layer_input, queries, keys, targets, value_weight)
    new_momentum = outer_mu * outer_momentum + mean_delta
    new_weight = value_weight - outer_rate * (mean_delta + outer_mu * new_momentum)
    return (new_weight, new_momentum)


def solution(mesh):
    in_specs = (
        P(None, ("replica", "fsdp"), None),
        P(None, ("replica", "fsdp"), None),
        P(None, ("replica", "fsdp"), None),
        P(None, ("replica", "fsdp"), None),
        P("fsdp", None),
        P("fsdp", None),
    )
    out_specs = (P("fsdp", None), P("fsdp", None))
    return jax.shard_map(shards, mesh=mesh, in_specs=in_specs, out_specs=out_specs, check_vma=False)
```
